32 devices in a mesh: gx: 8 (over y, x, core), gy: 4 (over z).
Axes of the slice: x: 2, y: 2, z: 4, core: 2. Of those that a mesh axis runs over, the one named last changes fastest.
Arguments:
- features: bfloat16 [32, 16, 128, 128], P(None, 'gx', 'gy'), may hold values from -80 to 80
- kernel_one: bfloat16 [32, 32, 3, 3, 3], replicated, may hold values from -0.21875 to 0.21875
- gain_one: float32 [32], replicated, may hold values from 0.5 to 1.5
- bias_one: float32 [32], replicated, may hold values from -0.5 to 0.5
- kernel_two: bfloat16 [32, 32, 3, 3, 3], replicated, may hold values from -0.21875 to 0.21875
- gain_two: float32 [32], replicated, may hold values from 0.5 to 1.5
- bias_two: float32 [32], replicated, may hold values from -0.5 to 0.5
- cotangent: bfloat16 [32, 16, 128, 128], P(None, 'gx', 'gy'), may hold values from -80 to 80
Outputs:
- output: bfloat16 [32, 16, 128, 128], P(None, 'gx', 'gy')
- features_grad: bfloat16 [32, 16, 128, 128], P(None, 'gx', 'gy')
- kernel_one_grad: float32 [32, 32, 3, 3, 3], replicated
- kernel_two_grad: float32 [32, 32, 3, 3, 3], replicated
- norm_grads: float32 [4, 32], replicated
The draws below stay inside these ranges and needn't reach their ends.
All inputs are finite; a program needn't handle non-finite values.
Results may differ from the reference program's by a relative error of at most 0.0078.
Values may be sent and summed in bfloat16 or wider, within the bound.
A program may use at most 192 MiB of HBM per device.

```python
import jax
import jax.numpy as jnp
from jax import lax

C = 32
NX = 16
NY = 128
NZ = 128


def scaled_volume(key, salt):
    key = jax.random.fold_in(key, salt)
    noise_key, offset_key, rough_key = jax.random.split(key, 3)
    offsets = jax.random.uniform(offset_key, (C, 1, 1, 1), jnp.float32, -1.0, 1.0)
    rough = jnp.exp(jax.random.uniform(rough_key, (C, NX, NY, NZ), jnp.float32, jnp.log(0.5), jnp.log(2.0)))
    place_x = jnp.arange(NX, dtype=jnp.float32) / NX
    place_y = jnp.arange(NY, dtype=jnp.float32) / NY
    noise = jnp.clip(jax.random.normal(noise_key, (C, NX, NY, NZ), jnp.float32), -4.0, 4.0)
    ramp = jnp.exp(jnp.log(3.0) * place_x)[:, None] * jnp.exp(jnp.log(2.0) * place_y)[None, :]
    return (noise + offsets) * rough * ramp[None, :, :, None]


def draw_features(key, part):
    return scaled_volume(key, 11).astype(jnp.bfloat16)


def draw_cotangent(key, part):
    return scaled_volume(key, 23).astype(jnp.bfloat16)


def scatter_about(stream_key, extent, width, limit, kind=jnp.bfloat16):
    drawn = width * jax.random.normal(stream_key, extent, jnp.float32)
    return jnp.clip(drawn, min=-limit, max=limit).astype(kind)


def setup_inputs(seed: int = 0) -> dict:
    keys = jax.random.split(jax.random.key(seed), 9)
    return {
        "features": draw_features(jax.random.fold_in(keys[8], 71), 0),
        "kernel_one": scatter_about(keys[1], (C, C, 3, 3, 3), (C * 27) ** -0.5, 0.21875),
        "gain_one": jnp.clip(1.0 + 0.1 * jax.random.normal(keys[2], (C,), jnp.float32), 0.5, 1.5),
        "bias_one": jnp.clip(jax.random.uniform(keys[3], (C,), jnp.float32, -0.5, 0.5), -0.5, 0.5),
        "kernel_two": scatter_about(keys[4], (C, C, 3, 3, 3), (C * 27) ** -0.5, 0.21875),
        "gain_two": jnp.clip(1.0 + 0.1 * jax.random.normal(keys[5], (C,), jnp.float32), 0.5, 1.5),
        "bias_two": jnp.clip(jax.random.uniform(keys[6], (C,), jnp.float32, -0.5, 0.5), -0.5, 0.5),
        "cotangent": draw_cotangent(jax.random.fold_in(keys[8], 71), 0),
    }


EPSILON = 1e-05
SLOPE = 0.01
SHARPNESS = 8.0

def activate(shifted):
    return SLOPE * shifted + (1.0 - SLOPE) * jax.nn.softplus(SHARPNESS * shifted) / SHARPNESS

def activate_slope(shifted):
    return SLOPE + (1.0 - SLOPE) * jax.nn.sigmoid(SHARPNESS * shifted)

def column(values):
    return values[:, None, None, None]

def pad_all(values):
    return jnp.pad(values, ((0, 0), (1, 1), (1, 1), (1, 1)))

def conv_valid(padded, kernel):
    result = lax.conv_general_dilated(padded[None], kernel, (1, 1, 1), 'VALID', dimension_numbers=('NCDHW', 'OIDHW', 'NCDHW'), preferred_element_type=jnp.float32)
    return result[0]

def flip_kernel(kernel):
    return jnp.transpose(kernel[:, :, ::-1, ::-1, ::-1], (1, 0, 2, 3, 4))

def weight_grad(padded, gradient):
    result = lax.conv_general_dilated(padded[:, None], gradient[:, None], (1, 1, 1), 'VALID', dimension_numbers=('NCDHW', 'OIDHW', 'NCDHW'), preferred_element_type=jnp.float32)
    return jnp.transpose(result, (1, 0, 2, 3, 4))

def normalize(hidden, total_cells):
    center = lax.optimization_barrier(jnp.sum(hidden, axis=(1, 2, 3))) / total_cells
    spread = lax.optimization_barrier(jnp.sum(jnp.square(hidden - column(center)), axis=(1, 2, 3))) / total_cells
    inverse_std = lax.rsqrt(spread + EPSILON)
    return ((hidden - column(center)) * column(inverse_std), inverse_std)

def norm_backward(slope, normed, gain, inverse_std, total_cells):
    sum_plain = lax.optimization_barrier(jnp.sum(slope, axis=(1, 2, 3)))
    sum_normed = lax.optimization_barrier(jnp.sum(slope * normed, axis=(1, 2, 3)))
    gradient = column(gain * inverse_std) * (slope - column(sum_plain / total_cells) - normed * column(sum_normed / total_cells))
    return (gradient.astype(jnp.bfloat16), sum_plain, sum_normed)

def reference(features, kernel_one, gain_one, bias_one, kernel_two, gain_two, bias_two, cotangent):
    total_cells = float(NX * NY * NZ)
    x_pad = pad_all(features)
    normed_one, inv_one = normalize(conv_valid(x_pad, kernel_one), total_cells)
    shifted_one = normed_one * column(gain_one) + column(bias_one)
    active = activate(shifted_one).astype(jnp.bfloat16)
    a_pad = pad_all(active)
    normed_two, inv_two = normalize(conv_valid(a_pad, kernel_two), total_cells)
    shifted_two = normed_two * column(gain_two) + column(bias_two)
    output = activate(shifted_two).astype(jnp.bfloat16)
    slope_two = cotangent.astype(jnp.float32) * activate_slope(shifted_two)
    grad_two, plain_two, nsum_two = norm_backward(slope_two, normed_two, gain_two, inv_two, total_cells)
    scale = 1.0 / jnp.sqrt(jnp.float32(total_cells))
    kernel_two_grad = weight_grad(a_pad, grad_two) * scale
    back_one = conv_valid(pad_all(grad_two), flip_kernel(kernel_two))
    slope_one = back_one * activate_slope(shifted_one)
    grad_one, plain_one, nsum_one = norm_backward(slope_one, normed_one, gain_one, inv_one, total_cells)
    kernel_one_grad = weight_grad(x_pad, grad_one) * scale
    features_grad = conv_valid(pad_all(grad_one), flip_kernel(kernel_one)).astype(jnp.bfloat16)
    norm_grads = jnp.stack([nsum_one, plain_one, nsum_two, plain_two]) * scale
    return (output, features_grad, kernel_one_grad, kernel_two_grad, norm_grads)
```

```python
import functools

import jax
import jax.numpy as jnp
from jax import lax
from jax.experimental import pallas as pl
from jax.experimental.pallas import tpu as pltpu
from jax.sharding import PartitionSpec as P

EPSILON = 1e-05
SLOPE = 0.01
SHARPNESS = 8.0
MESH = pl.DeviceIdType.MESH
F32 = jnp.float32
BF16 = jnp.bfloat16
VSPEC = pl.BlockSpec(memory_space=pltpu.VMEM)
DIRECTIONS = [(i, j) for i in (-1, 0, 1) for j in (-1, 0, 1) if (i, j) != (0, 0)]


def activate(shifted):
    scaled = SHARPNESS * shifted
    soft = jnp.maximum(scaled, 0.0) + jnp.log1p(jnp.exp(-jnp.abs(scaled)))
    return SLOPE * shifted + (1.0 - SLOPE) * soft / SHARPNESS


def activate_slope(shifted):
    return SLOPE + (1.0 - SLOPE) / (1.0 + jnp.exp(-SHARPNESS * shifted))


def halo_kernel(nx, ny, t_ref, o_ref, p_ref, send, recv):
    gx, gy = lax.axis_index("gx"), lax.axis_index("gy")
    X, Y = t_ref.shape[0], t_ref.shape[1]
    peers = [(lax.rem(gx + dx + nx, nx), lax.rem(gy + dy + ny, ny)) for dx, dy in DIRECTIONS]
    barrier = pltpu.get_barrier_semaphore()
    for peer in peers:
        pl.semaphore_signal(barrier, inc=1, device_id=peer, device_id_type=MESH)
    pl.semaphore_wait(barrier, len(peers))

    def source(d, size):
        return pl.ds(size - 1, 1) if d == 1 else (pl.ds(0, 1) if d == -1 else pl.ds(0, size))

    def target(d, size):
        return pl.ds(0, 1) if d == 1 else (pl.ds(size + 1, 1) if d == -1 else pl.ds(1, size))

    copies = []
    for k, (dx, dy) in enumerate(DIRECTIONS):
        copy = pltpu.make_async_remote_copy(
            src_ref=t_ref.at[source(dx, X), source(dy, Y)],
            dst_ref=p_ref.at[target(dx, X), target(dy, Y)],
            send_sem=send.at[k],
            recv_sem=recv.at[k],
            device_id=peers[k],
            device_id_type=MESH,
        )
        copy.start()
        copies.append(copy)
    o_ref[1 : X + 1, 1 : Y + 1] = t_ref[...]
    for copy in copies:
        copy.wait()
    low_x = jnp.where(gx > 0, 1.0, 0.0)
    high_x = jnp.where(gx < nx - 1, 1.0, 0.0)
    low_y = jnp.where(gy > 0, 1.0, 0.0)
    high_y = jnp.where(gy < ny - 1, 1.0, 0.0)

    def kept(values, flag):
        return (values.astype(F32) * flag).astype(BF16)

    o_ref[0, 1 : Y + 1] = kept(p_ref[0, 1 : Y + 1], low_x)
    o_ref[X + 1, 1 : Y + 1] = kept(p_ref[X + 1, 1 : Y + 1], high_x)
    for x in range(X + 2):
        side = low_x if x == 0 else (high_x if x == X + 1 else None)
        low = low_y if side is None else low_y * side
        high = high_y if side is None else high_y * side
        o_ref[x, 0] = kept(p_ref[x, 0], low)
        o_ref[x, Y + 1] = kept(p_ref[x, Y + 1], high)


def halo(block, nx, ny):
    X, Y, C, Z = block.shape
    return pl.pallas_call(
        functools.partial(halo_kernel, nx, ny),
        name="halo",
        out_shape=jax.ShapeDtypeStruct((X + 2, Y + 2, C, Z), block.dtype),
        in_specs=[VSPEC],
        out_specs=VSPEC,
        scratch_shapes=[
            pltpu.VMEM((X + 2, Y + 2, C, Z), block.dtype),
            pltpu.SemaphoreType.DMA((8,)),
            pltpu.SemaphoreType.DMA((8,)),
        ],
        compiler_params=pltpu.CompilerParams(collective_id=0, has_side_effects=True),
    )(block)


def greet(nx, ny, gx, gy):
    barrier = pltpu.get_barrier_semaphore()
    for k in range(1, nx):
        peer = (lax.rem(gx + k, nx), gy)
        pl.semaphore_signal(barrier, inc=1, device_id=peer, device_id_type=MESH)
    for k in range(1, ny):
        peer = (gx, lax.rem(gy + k, ny))
        pl.semaphore_signal(barrier, inc=1, device_id=peer, device_id_type=MESH)
    pl.semaphore_wait(barrier, nx + ny - 2)


def spread(count, me, peer_of, source_of, slots, send, recv):
    copies = []
    for k in range(1, count):
        other = lax.rem(me + k, count)
        copy = pltpu.make_async_remote_copy(
            src_ref=source_of(other),
            dst_ref=slots(me),
            send_sem=send.at[k],
            recv_sem=recv.at[me],
            device_id=peer_of(other),
            device_id_type=MESH,
        )
        copy.start()
        copies.append(copy)
    for k in range(1, count):
        other = lax.rem(me + k, count)
        pltpu.make_async_remote_copy(
            src_ref=source_of(other),
            dst_ref=slots(other),
            send_sem=send.at[k],
            recv_sem=recv.at[other],
            device_id=peer_of(other),
            device_id_type=MESH,
        ).wait_recv()
    for copy in copies:
        copy.wait_send()


def ordered_sum(ref, count):
    total = ref[0]
    for k in range(1, count):
        total = total + ref[k]
    return total


def stats_kernel(nx, ny, s_ref, o_ref, bx, by, mid, sx, rx, sy, ry):
    gx, gy = lax.axis_index("gx"), lax.axis_index("gy")
    greet(nx, ny, gx, gy)
    bx[gx] = s_ref[...]
    spread(nx, gx, lambda o: (o, gy), lambda o: s_ref, lambda i: bx.at[i], sx, rx)
    mid[...] = ordered_sum(bx, nx)
    by[gy] = mid[...]
    spread(ny, gy, lambda o: (gx, o), lambda o: mid, lambda i: by.at[i], sy, ry)
    o_ref[...] = ordered_sum(by, ny)


def sum_stats(local, nx, ny):
    R, L = local.shape
    return pl.pallas_call(
        functools.partial(stats_kernel, nx, ny),
        name="stats_sum",
        out_shape=jax.ShapeDtypeStruct((R, L), F32),
        in_specs=[VSPEC],
        out_specs=VSPEC,
        scratch_shapes=[
            pltpu.VMEM((nx, R, L), F32),
            pltpu.VMEM((ny, R, L), F32),
            pltpu.VMEM((R, L), F32),
            pltpu.SemaphoreType.DMA((nx,)),
            pltpu.SemaphoreType.DMA((nx,)),
            pltpu.SemaphoreType.DMA((ny,)),
            pltpu.SemaphoreType.DMA((ny,)),
        ],
        compiler_params=pltpu.CompilerParams(collective_id=1, has_side_effects=True),
    )(local)


def weights_kernel(nx, ny, s_ref, o_ref, bx, by, mid, fin, gat, sx, rx, sy, ry, sg, rg):
    gx, gy = lax.axis_index("gx"), lax.axis_index("gy")
    greet(nx, ny, gx, gy)
    bx[gx] = s_ref[gx]
    spread(nx, gx, lambda o: (o, gy), lambda o: s_ref.at[o], lambda i: bx.at[i], sx, rx)
    mid[...] = ordered_sum(bx, nx)
    by[gy] = mid[...]
    spread(ny, gy, lambda o: (gx, o), lambda o: mid, lambda i: by.at[i], sy, ry)
    fin[...] = ordered_sum(by, ny)
    gat[gx] = fin[...]
    spread(nx, gx, lambda o: (o, gy), lambda o: fin, lambda i: gat.at[i], sg, rg)
    o_ref[...] = gat[...]


def sum_weights(local, nx, ny):
    R, L = local.shape
    piece = -(-R // (8 * nx)) * 8
    split = jnp.pad(local, ((0, piece * nx - R), (0, 0))).reshape(nx, piece, L)
    summed = pl.pallas_call(
        functools.partial(weights_kernel, nx, ny),
        name="weights_sum",
        out_shape=jax.ShapeDtypeStruct((nx, piece, L), F32),
        in_specs=[VSPEC],
        out_specs=VSPEC,
        scratch_shapes=[
            pltpu.VMEM((nx, piece, L), F32),
            pltpu.VMEM((ny, piece, L), F32),
            pltpu.VMEM((piece, L), F32),
            pltpu.VMEM((piece, L), F32),
            pltpu.VMEM((nx, piece, L), F32),
            pltpu.SemaphoreType.DMA((nx,)),
            pltpu.SemaphoreType.DMA((nx,)),
            pltpu.SemaphoreType.DMA((ny,)),
            pltpu.SemaphoreType.DMA((ny,)),
            pltpu.SemaphoreType.DMA((nx,)),
            pltpu.SemaphoreType.DMA((nx,)),
        ],
        compiler_params=pltpu.CompilerParams(collective_id=2, has_side_effects=True),
    )(split)
    return summed.reshape(nx * piece, L)[:R]


def taps(row):
    wide = row.astype(F32)
    size = row.shape[1]
    lane = lax.broadcasted_iota(jnp.int32, wide.shape, 1)
    before = jnp.where(lane == 0, 0.0, pltpu.roll(wide, 1, 1)).astype(BF16)
    after = jnp.where(lane == size - 1, 0.0, pltpu.roll(wide, size - 1, 1)).astype(BF16)
    return jnp.concatenate([before, row, after], axis=0)


def conv_rows(p_ref, w_ref, acc_ref, v_ref=None, dw_ref=None):
    X = acc_ref.shape[0]
    C = acc_ref.shape[2]
    Z = acc_ref.shape[3]
    acc_ref[...] = jnp.zeros_like(acc_ref)
    if dw_ref is not None:
        dw_ref[...] = jnp.zeros_like(dw_ref)

    def body(j, carry):
        y = 2 * j
        for xp in range(X + 2):
            first, last = max(0, xp - (X - 1)), min(2, xp)
            pair = jnp.concatenate([taps(p_ref[xp, y]), taps(p_ref[xp, y + 1])], axis=1)
            part = jnp.dot(
                w_ref[first * 3 * C : (last + 1) * 3 * C, :], pair, preferred_element_type=F32
            )
            for dx in range(first, last + 1):
                base = (dx - first) * 3 * C
                one = [part[base + d * C : base + (d + 1) * C, :Z] for d in range(3)]
                two = [part[base + d * C : base + (d + 1) * C, Z:] for d in range(3)]
                x = xp - dx
                acc_ref[x, y] += one[2]
                acc_ref[x, y + 1] += one[1] + two[2]
                acc_ref[x, y + 2] += one[0] + two[1]
                acc_ref[x, y + 3] += two[0]
            if dw_ref is not None:
                left = []
                for dx in range(first, last + 1):
                    x = xp - dx
                    now = v_ref[x, pl.ds(y, 3)].reshape(3 * C, Z)
                    later = v_ref[x, pl.ds(y + 1, 3)].reshape(3 * C, Z)
                    left.append(jnp.concatenate([now, later], axis=1))
                left = left[0] if len(left) == 1 else jnp.concatenate(left, axis=0)
                dw_ref[first * 3 * C : (last + 1) * 3 * C, : 3 * C] += lax.dot_general(
                    left, pair, (((1,), (1,)), ((), ())), preferred_element_type=F32
                )
        return carry

    lax.fori_loop(0, p_ref.shape[1] // 2, body, 0)


def pack_pair(one, two):
    lane = lax.broadcasted_iota(jnp.int32, one.shape, 1)
    one = jnp.sum(one, axis=1, keepdims=True)
    two = jnp.sum(two, axis=1, keepdims=True)
    return jnp.where(lane == 0, one, jnp.where(lane == 1, two, 0.0))


def normal_terms(s_ref, total_cells):
    center = s_ref[:, 0:1] / total_cells
    spread_ = s_ref[:, 1:2] / total_cells - jnp.square(center)
    return center, lax.rsqrt(spread_ + EPSILON)


def rows(X, Y, step, carry):
    group = 4 if Y % 4 == 0 else 1

    def body(block, carry):
        for k in range(group):
            for x in range(X):
                carry = step(x, block * group + k, carry)
        return carry

    return lax.fori_loop(0, Y // group, body, carry)


def forward_kernel(p_ref, w_ref, h_ref, s_ref, acc_ref):
    X, Y, C, Z = h_ref.shape
    conv_rows(p_ref, w_ref, acc_ref)

    def step(x, y, carry):
        h = acc_ref[x, y + 2]
        h_ref[x, y] = h
        return carry[0] + h, carry[1] + h * h

    zero = jnp.zeros((C, Z), F32)
    s_ref[...] = pack_pair(*rows(X, Y, step, (zero, zero)))


def active_kernel(total_cells, h_ref, s_ref, gb_ref, a_ref):
    X, Y, C, Z = h_ref.shape
    center, inverse = normal_terms(s_ref, total_cells)
    gain, bias = gb_ref[0], gb_ref[1]

    def step(x, y, carry):
        shifted = (h_ref[x, y] - center) * inverse * gain + bias
        a_ref[x, y] = activate(shifted).astype(BF16)
        return carry

    rows(X, Y, step, 0)


def output_kernel(total_cells, h_ref, s_ref, gb_ref, c_ref, o_ref, t_ref):
    X, Y, C, Z = h_ref.shape
    center, inverse = normal_terms(s_ref, total_cells)
    gain, bias = gb_ref[0], gb_ref[1]

    def step(x, y, carry):
        normed = (h_ref[x, y] - center) * inverse
        shifted = normed * gain + bias
        o_ref[x, y] = activate(shifted).astype(BF16)
        slope = c_ref[x, y].astype(F32) * activate_slope(shifted)
        return carry[0] + slope, carry[1] + slope * normed

    zero = jnp.zeros((C, Z), F32)
    t_ref[...] = pack_pair(*rows(X, Y, step, (zero, zero)))


def gradient_kernel(total_cells, has_slope, h_ref, s_ref, gb_ref, c_ref, t_ref, g_ref):
    X, Y, C, Z = h_ref.shape
    center, inverse = normal_terms(s_ref, total_cells)
    gain, bias = gb_ref[0], gb_ref[1]
    plain = t_ref[:, 0:1] / total_cells
    along = t_ref[:, 1:2] / total_cells
    factor = gain * inverse

    def step(x, y, carry):
        normed = (h_ref[x, y] - center) * inverse
        slope = c_ref[x, y].astype(F32)
        if not has_slope:
            slope = slope * activate_slope(normed * gain + bias)
        g_ref[x, y] = (factor * (slope - plain - normed * along)).astype(BF16)
        return carry

    rows(X, Y, step, 0)


def fill_own(v_ref, own_ref):
    X, Y, C, Z = v_ref.shape
    edge = jnp.zeros((X, 2, C, Z), BF16)
    own_ref[:, 0:2] = edge
    own_ref[:, Y + 2 : Y + 4] = edge
    own_ref[:, 2 : Y + 2] = v_ref[...]


def back_kernel(
    total_cells, p_ref, v_ref, w_ref, h_ref, s_ref, gb_ref, o_ref, t_ref, dw_ref, acc_ref, own_ref
):
    X, Y, C, Z = o_ref.shape
    fill_own(v_ref, own_ref)
    conv_rows(p_ref, w_ref, acc_ref, own_ref, dw_ref)
    center, inverse = normal_terms(s_ref, total_cells)
    gain, bias = gb_ref[0], gb_ref[1]

    def step(x, y, carry):
        normed = (h_ref[x, y] - center) * inverse
        slope = acc_ref[x, y + 2] * activate_slope(normed * gain + bias)
        o_ref[x, y] = slope
        return carry[0] + slope, carry[1] + slope * normed

    zero = jnp.zeros((C, Z), F32)
    t_ref[...] = pack_pair(*rows(X, Y, step, (zero, zero)))


def last_kernel(p_ref, v_ref, w_ref, o_ref, dw_ref, acc_ref, own_ref):
    X, Y, C, Z = o_ref.shape
    fill_own(v_ref, own_ref)
    conv_rows(p_ref, w_ref, acc_ref, own_ref, dw_ref)

    def step(x, y, carry):
        o_ref[x, y] = acc_ref[x, y + 2].astype(BF16)
        return carry

    rows(X, Y, step, 0)


def call(kernel, name, outs, *operands, scratch=()):
    return pl.pallas_call(
        kernel,
        name=name,
        out_shape=[jax.ShapeDtypeStruct(s, d) for s, d in outs],
        in_specs=[VSPEC] * len(operands),
        out_specs=[VSPEC] * len(outs),
        scratch_shapes=[pltpu.VMEM(s, d) for s, d in scratch],
    )(*operands)


def local(features, kernel_one, gain_one, bias_one, kernel_two, gain_two, bias_two, cotangent):
    C, X, Y, Z = features.shape
    nx, ny = lax.axis_size("gx"), lax.axis_size("gy")
    total_cells = float(X * Y * Z * nx * ny)
    full = (X, Y, C, Z)
    tall = (X, Y + 4, C, Z)
    stat = (C, 128)

    def ahead(kernel):
        return jnp.transpose(kernel, (2, 3, 0, 4, 1)).reshape(9 * C, 3 * C)

    def behind(kernel):
        return jnp.transpose(kernel[:, :, ::-1, ::-1, ::-1], (2, 3, 1, 4, 0)).reshape(9 * C, 3 * C)

    def rows_of(gain, bias):
        return jnp.broadcast_to(jnp.stack([gain, bias])[:, :, None], (2, C, Z))

    params_one, params_two = rows_of(gain_one, bias_one), rows_of(gain_two, bias_two)
    ft = jnp.transpose(features, (1, 2, 0, 3))
    ct = jnp.transpose(cotangent, (1, 2, 0, 3))

    h1, s1 = call(
        forward_kernel, "forward", [(full, F32), (stat, F32)], halo(ft, nx, ny),
        ahead(kernel_one), scratch=[(tall, F32)],
    )
    s1 = sum_stats(s1, nx, ny)
    (a,) = call(
        functools.partial(active_kernel, total_cells), "active", [(full, BF16)], h1, s1, params_one
    )
    h2, s2 = call(
        forward_kernel, "forward", [(full, F32), (stat, F32)], halo(a, nx, ny),
        ahead(kernel_two), scratch=[(tall, F32)],
    )
    s2 = sum_stats(s2, nx, ny)
    out, t2 = call(
        functools.partial(output_kernel, total_cells), "output", [(full, BF16), (stat, F32)],
        h2, s2, params_two, ct,
    )
    t2 = sum_stats(t2, nx, ny)
    (g2,) = call(
        functools.partial(gradient_kernel, total_cells, False), "grad_two", [(full, BF16)],
        h2, s2, params_two, ct, t2,
    )
    slope_one, t1, dw2 = call(
        functools.partial(back_kernel, total_cells), "back",
        [(full, F32), (stat, F32), ((9 * C, 128), F32)],
        halo(g2, nx, ny), a, behind(kernel_two), h1, s1, params_one,
        scratch=[(tall, F32), (tall, BF16)],
    )
    t1 = sum_stats(t1, nx, ny)
    (g1,) = call(
        functools.partial(gradient_kernel, total_cells, True), "grad_one", [(full, BF16)],
        h1, s1, params_one, slope_one, t1,
    )
    fg, dw1 = call(
        last_kernel, "last", [(full, BF16), ((9 * C, 128), F32)],
        halo(g1, nx, ny), ft, behind(kernel_one), scratch=[(tall, F32), (tall, BF16)],
    )
    summed = sum_weights(jnp.concatenate([dw1, dw2], axis=0), nx, ny)
    scale = 1.0 / jnp.sqrt(jnp.float32(total_cells))

    def gradient_of(block):
        split = block[:, : 3 * C].reshape(3, 3, C, 3, C)
        return jnp.transpose(split[::-1, :, :, ::-1, :], (4, 2, 0, 1, 3)) * scale

    norm_grads = jnp.stack([t1[:, 1], t1[:, 0], t2[:, 1], t2[:, 0]]) * scale
    return (
        jnp.transpose(out, (2, 0, 1, 3)),
        jnp.transpose(fg, (2, 0, 1, 3)),
        gradient_of(summed[: 9 * C]),
        gradient_of(summed[9 * C :]),
        norm_grads,
    )


def solution(mesh):
    in_specs = (P(None, "gx", "gy", None), P(), P(), P(), P(), P(), P(), P(None, "gx", "gy", None))
    out_specs = (P(None, "gx", "gy", None), P(None, "gx", "gy", None), P(), P(), P())
    return jax.shard_map(local, mesh=mesh, in_specs=in_specs, out_specs=out_specs, check_vma=False)
```

```python
import functools

import jax
import jax.numpy as jnp
from jax import lax
from jax.experimental import pallas as pl
from jax.experimental.pallas import tpu as pltpu
from jax.sharding import PartitionSpec as P

EPSILON = 1e-05
SLOPE = 0.01
SHARPNESS = 8.0
MESH = pl.DeviceIdType.MESH
F32 = jnp.float32
BF16 = jnp.bfloat16
VSPEC = pl.BlockSpec(memory_space=pltpu.VMEM)
PIECES = 4
DIRECTIONS = [(i, j) for i in (-1, 0, 1) for j in (-1, 0, 1) if (i, j) != (0, 0)]


def activate(shifted):
    scaled = SHARPNESS * shifted
    soft = jnp.maximum(scaled, 0.0) + jnp.log1p(jnp.exp(-jnp.abs(scaled)))
    return SLOPE * shifted + (1.0 - SLOPE) * soft / SHARPNESS


def activate_slope(shifted):
    return SLOPE + (1.0 - SLOPE) / (1.0 + jnp.exp(-SHARPNESS * shifted))


def start_halo(nx, ny, t_ref, p_ref, send, recv):
    gx, gy = lax.axis_index("gx"), lax.axis_index("gy")
    X, Y = t_ref.shape[0], t_ref.shape[1]
    peers = [(lax.rem(gx + dx + nx, nx), lax.rem(gy + dy + ny, ny)) for dx, dy in DIRECTIONS]
    barrier = pltpu.get_barrier_semaphore()
    for peer in peers:
        pl.semaphore_signal(barrier, inc=1, device_id=peer, device_id_type=MESH)
    pl.semaphore_wait(barrier, len(peers))

    def source(d, size):
        return pl.ds(size - 1, 1) if d == 1 else (pl.ds(0, 1) if d == -1 else pl.ds(0, size))

    def target(d, size):
        return pl.ds(0, 1) if d == 1 else (pl.ds(size + 1, 1) if d == -1 else pl.ds(1, size))

    piece = Y // PIECES
    plan = []
    for n in range(PIECES):
        for k, (dx, dy) in enumerate(DIRECTIONS):
            if dy == 0:
                rows_from, rows_to = pl.ds(n * piece, piece), pl.ds(n * piece + 1, piece)
                plan.append((n, k, dx, rows_from, rows_to))
            elif n == 0:
                plan.append((n, k, dx, source(dy, Y), target(dy, Y)))
    groups = [[] for _ in range(PIECES)]
    for index, (n, k, dx, rows_from, rows_to) in enumerate(plan):
        copy = pltpu.make_async_remote_copy(
            src_ref=t_ref.at[source(dx, X), rows_from],
            dst_ref=p_ref.at[target(dx, X), rows_to],
            send_sem=send.at[index],
            recv_sem=recv.at[index],
            device_id=peers[k],
            device_id_type=MESH,
        )
        copy.start()
        groups[n].append(copy)
    return groups


def greet(nx, ny, gx, gy):
    barrier = pltpu.get_barrier_semaphore()
    for k in range(1, nx):
        peer = (lax.rem(gx + k, nx), gy)
        pl.semaphore_signal(barrier, inc=1, device_id=peer, device_id_type=MESH)
    for k in range(1, ny):
        peer = (gx, lax.rem(gy + k, ny))
        pl.semaphore_signal(barrier, inc=1, device_id=peer, device_id_type=MESH)
    pl.semaphore_wait(barrier, nx + ny - 2)


def spread(count, me, peer_of, source_of, slots, send, recv):
    copies = []
    for k in range(1, count):
        other = lax.rem(me + k, count)
        copy = pltpu.make_async_remote_copy(
            src_ref=source_of(other),
            dst_ref=slots(me),
            send_sem=send.at[k],
            recv_sem=recv.at[me],
            device_id=peer_of(other),
            device_id_type=MESH,
        )
        copy.start()
        copies.append(copy)
    for k in range(1, count):
        other = lax.rem(me + k, count)
        pltpu.make_async_remote_copy(
            src_ref=source_of(other),
            dst_ref=slots(other),
            send_sem=send.at[k],
            recv_sem=recv.at[other],
            device_id=peer_of(other),
            device_id_type=MESH,
        ).wait_recv()
    for copy in copies:
        copy.wait_send()


def ordered_sum(ref, count):
    total = ref[0]
    for k in range(1, count):
        total = total + ref[k]
    return total


def stats_kernel(nx, ny, s_ref, o_ref, bx, by, mid, sx, rx, sy, ry):
    gx, gy = lax.axis_index("gx"), lax.axis_index("gy")
    greet(nx, ny, gx, gy)
    bx[gx] = s_ref[...]
    spread(nx, gx, lambda o: (o, gy), lambda o: s_ref, lambda i: bx.at[i], sx, rx)
    mid[...] = ordered_sum(bx, nx)
    by[gy] = mid[...]
    spread(ny, gy, lambda o: (gx, o), lambda o: mid, lambda i: by.at[i], sy, ry)
    o_ref[...] = ordered_sum(by, ny)


def sum_stats(local, nx, ny):
    R, L = local.shape
    return pl.pallas_call(
        functools.partial(stats_kernel, nx, ny),
        name="stats_sum",
        out_shape=jax.ShapeDtypeStruct((R, L), F32),
        in_specs=[VSPEC],
        out_specs=VSPEC,
        scratch_shapes=[
            pltpu.VMEM((nx, R, L), F32),
            pltpu.VMEM((ny, R, L), F32),
            pltpu.VMEM((R, L), F32),
            pltpu.SemaphoreType.DMA((nx,)),
            pltpu.SemaphoreType.DMA((nx,)),
            pltpu.SemaphoreType.DMA((ny,)),
            pltpu.SemaphoreType.DMA((ny,)),
        ],
        compiler_params=pltpu.CompilerParams(collective_id=1, has_side_effects=True),
    )(local)


def weights_kernel(nx, ny, s_ref, o_ref, bx, by, mid, fin, gat, sx, rx, sy, ry, sg, rg):
    gx, gy = lax.axis_index("gx"), lax.axis_index("gy")
    greet(nx, ny, gx, gy)
    bx[gx] = s_ref[gx]
    spread(nx, gx, lambda o: (o, gy), lambda o: s_ref.at[o], lambda i: bx.at[i], sx, rx)
    mid[...] = ordered_sum(bx, nx)
    by[gy] = mid[...]
    spread(ny, gy, lambda o: (gx, o), lambda o: mid, lambda i: by.at[i], sy, ry)
    fin[...] = ordered_sum(by, ny)
    gat[gx] = fin[...]
    spread(nx, gx, lambda o: (o, gy), lambda o: fin, lambda i: gat.at[i], sg, rg)
    o_ref[...] = gat[...]


def sum_weights(local, nx, ny):
    R, L = local.shape
    piece = -(-R // (8 * nx)) * 8
    split = jnp.pad(local, ((0, piece * nx - R), (0, 0))).reshape(nx, piece, L)
    summed = pl.pallas_call(
        functools.partial(weights_kernel, nx, ny),
        name="weights_sum",
        out_shape=jax.ShapeDtypeStruct((nx, piece, L), F32),
        in_specs=[VSPEC],
        out_specs=VSPEC,
        scratch_shapes=[
            pltpu.VMEM((nx, piece, L), F32),
            pltpu.VMEM((ny, piece, L), F32),
            pltpu.VMEM((piece, L), F32),
            pltpu.VMEM((piece, L), F32),
            pltpu.VMEM((nx, piece, L), F32),
            pltpu.SemaphoreType.DMA((nx,)),
            pltpu.SemaphoreType.DMA((nx,)),
            pltpu.SemaphoreType.DMA((ny,)),
            pltpu.SemaphoreType.DMA((ny,)),
            pltpu.SemaphoreType.DMA((nx,)),
            pltpu.SemaphoreType.DMA((nx,)),
        ],
        compiler_params=pltpu.CompilerParams(collective_id=2, has_side_effects=True),
    )(split)
    return summed.reshape(nx * piece, L)[:R]


def taps(row, flip, keep=None):
    wide = row.astype(F32)
    if keep is not None:
        wide = wide * keep
        row = wide.astype(BF16)
    size = row.shape[1]
    lane = lax.broadcasted_iota(jnp.int32, wide.shape, 1)
    before = jnp.where(lane == 0, 0.0, pltpu.roll(wide, 1, 1)).astype(BF16)
    after = jnp.where(lane == size - 1, 0.0, pltpu.roll(wide, size - 1, 1)).astype(BF16)
    return jnp.concatenate([after, row, before] if flip else [before, row, after], axis=0)


def conv_halo(nx, ny, flip, t_ref, w_ref, acc_ref, p_ref, send, recv, v_ref=None, dw_ref=None):
    X, _, C, Z = acc_ref.shape
    Y = t_ref.shape[1]
    gx, gy = lax.axis_index("gx"), lax.axis_index("gy")
    groups = start_halo(nx, ny, t_ref, p_ref, send, recv)
    acc_ref[...] = jnp.zeros_like(acc_ref)
    if dw_ref is not None:
        dw_ref[...] = jnp.zeros(dw_ref.shape, F32)

    def pair_step(xp, ya, yb, tap_a, tap_b):
        first, last = max(0, xp - (X - 1)), min(2, xp)
        blocks = range(2 - last, 3 - first) if flip else range(first, last + 1)
        low, high = blocks[0] * 3 * C, (blocks[-1] + 1) * 3 * C
        pair = jnp.concatenate([tap_a, tap_b], axis=1)
        part = jnp.dot(w_ref[low:high, :], pair, preferred_element_type=F32)
        left = []
        for n, block in enumerate(blocks):
            x = xp - 2 + block if flip else xp - block
            base = n * 3 * C
            one = [part[base + d * C : base + (d + 1) * C, :Z] for d in range(3)]
            two = [part[base + d * C : base + (d + 1) * C, Z:] for d in range(3)]
            if not flip:
                one, two = one[::-1], two[::-1]
            if yb is None:
                acc_ref[x, ya] += one[0]
                acc_ref[x, ya + 1] += one[1] + two[0]
                acc_ref[x, ya + 2] += one[2] + two[1]
                acc_ref[x, ya + 3] += two[2]
            else:
                for d in range(3):
                    acc_ref[x, ya + d] += one[d]
                for d in range(3):
                    acc_ref[x, yb + d] += two[d]
            if dw_ref is not None:
                second = ya + 1 if yb is None else yb
                now = v_ref[x, pl.ds(ya, 3)].reshape(3 * C, Z)
                later = v_ref[x, pl.ds(second, 3)].reshape(3 * C, Z)
                left.append(jnp.concatenate([now, later], axis=1))
        if dw_ref is not None:
            left = left[0] if len(left) == 1 else jnp.concatenate(left, axis=0)
            dw_ref[low:high, : 3 * C] += lax.dot_general(
                left, pair, (((1,), (1,)), ((), ())), preferred_element_type=F32
            )

    def inner(j, carry):
        y = 2 * j + 1
        for xp in range(1, X + 1):
            tap_a = taps(t_ref[xp - 1, y - 1], flip)
            tap_b = taps(t_ref[xp - 1, y], flip)
            pair_step(xp, y, None, tap_a, tap_b)
        return carry

    lax.fori_loop(0, Y // 2, inner, 0)
    for copy in groups[0]:
        copy.wait()
    low_y = jnp.where(gy > 0, 1.0, 0.0)
    high_y = jnp.where(gy < ny - 1, 1.0, 0.0)
    for xp in range(1, X + 1):
        tap_a = taps(p_ref[xp, 0], flip, low_y)
        tap_b = taps(p_ref[xp, Y + 1], flip, high_y)
        pair_step(xp, 0, Y + 1, tap_a, tap_b)
    low_x = jnp.where(gx > 0, 1.0, 0.0)
    high_x = jnp.where(gx < nx - 1, 1.0, 0.0)

    def outer(j, carry):
        y = 2 * j
        keep_a = jnp.where(y == 0, low_y, 1.0)
        keep_b = jnp.where(y == Y, high_y, 1.0)
        for xp, keep in ((0, low_x), (X + 1, high_x)):
            tap_a = taps(p_ref[xp, y], flip, keep * keep_a)
            tap_b = taps(p_ref[xp, y + 1], flip, keep * keep_b)
            pair_step(xp, y, None, tap_a, tap_b)
        return carry

    done = 0
    for n, group in enumerate(groups):
        if n > 0:
            for copy in group:
                copy.wait()
        ready = (Y + 2) // 2 if n == PIECES - 1 else (Y // PIECES * (n + 1) + 1) // 2
        lax.fori_loop(done, ready, outer, 0)
        done = ready


def pack_pair(one, two):
    C = one.shape[0]
    lane = lax.broadcasted_iota(jnp.int32, one.shape, 1)
    one = jnp.sum(one, axis=1, keepdims=True)
    two = jnp.sum(two, axis=1, keepdims=True)
    tall = jnp.where(lane == 0, one, jnp.where(lane == 1, two, 0.0))
    square = jnp.concatenate([tall, jnp.zeros((128 - C, 128), F32)], axis=0)
    return jnp.transpose(square)[0:8]


def unpack_pair(s_ref, C):
    square = jnp.concatenate([s_ref[...], jnp.zeros((120, 128), F32)], axis=0)
    tall = jnp.transpose(square)
    return tall[:C, 0:1], tall[:C, 1:2]


def normal_terms(s_ref, C, total_cells):
    sums, squares = unpack_pair(s_ref, C)
    center = sums / total_cells
    spread_ = squares / total_cells - jnp.square(center)
    return center, lax.rsqrt(spread_ + EPSILON)


def rows(X, Y, step, carry):
    group = 4 if Y % 4 == 0 else 1

    def body(block, carry):
        for k in range(group):
            for x in range(X):
                carry = step(x, block * group + k, carry)
        return carry

    return lax.fori_loop(0, Y // group, body, carry)


def forward_kernel(nx, ny, t_ref, w_ref, h_ref, s_ref, acc_ref, p_ref, send, recv):
    X, Y, C, Z = h_ref.shape
    conv_halo(nx, ny, False, t_ref, w_ref, acc_ref, p_ref, send, recv)

    def step(x, y, carry):
        h = acc_ref[x, y + 2]
        h_ref[x, y] = h
        return carry[0] + h, carry[1] + h * h

    zero = jnp.zeros((C, Z), F32)
    s_ref[...] = pack_pair(*rows(X, Y, step, (zero, zero)))


def active_kernel(total_cells, h_ref, s_ref, gb_ref, a_ref):
    X, Y, C, Z = h_ref.shape
    center, inverse = normal_terms(s_ref, C, total_cells)
    gain, bias = gb_ref[0], gb_ref[1]

    def step(x, y, carry):
        shifted = (h_ref[x, y] - center) * inverse * gain + bias
        a_ref[x, y] = activate(shifted).astype(BF16)
        return carry

    rows(X, Y, step, 0)


def output_kernel(total_cells, h_ref, s_ref, gb_ref, c_ref, o_ref, t_ref):
    X, Y, C, Z = h_ref.shape
    center, inverse = normal_terms(s_ref, C, total_cells)
    gain, bias = gb_ref[0], gb_ref[1]

    def step(x, y, carry):
        normed = (h_ref[x, y] - center) * inverse
        shifted = normed * gain + bias
        o_ref[x, y] = activate(shifted).astype(BF16)
        slope = c_ref[x, y].astype(F32) * activate_slope(shifted)
        return carry[0] + slope, carry[1] + slope * normed

    zero = jnp.zeros((C, Z), F32)
    t_ref[...] = pack_pair(*rows(X, Y, step, (zero, zero)))


def gradient_kernel(total_cells, has_slope, h_ref, s_ref, gb_ref, c_ref, t_ref, g_ref):
    X, Y, C, Z = h_ref.shape
    center, inverse = normal_terms(s_ref, C, total_cells)
    gain, bias = gb_ref[0], gb_ref[1]
    plain, along = [v / total_cells for v in unpack_pair(t_ref, C)]
    factor = gain * inverse

    def step(x, y, carry):
        normed = (h_ref[x, y] - center) * inverse
        slope = c_ref[x, y].astype(F32)
        if not has_slope:
            slope = slope * activate_slope(normed * gain + bias)
        g_ref[x, y] = (factor * (slope - plain - normed * along)).astype(BF16)
        return carry

    rows(X, Y, step, 0)


def fill_own(v_ref, own_ref):
    X, Y, C, Z = v_ref.shape
    edge = jnp.zeros((X, 2, C, Z), BF16)
    own_ref[:, 0:2] = edge
    own_ref[:, Y + 2 : Y + 4] = edge
    own_ref[:, 2 : Y + 2] = v_ref[...]


def back_kernel(
    total_cells, nx, ny, g_ref, v_ref, w_ref, h_ref, s_ref, gb_ref,
    o_ref, t_ref, dw_ref, acc_ref, p_ref, send, recv, own_ref,
):
    X, Y, C, Z = o_ref.shape
    fill_own(v_ref, own_ref)
    conv_halo(nx, ny, True, g_ref, w_ref, acc_ref, p_ref, send, recv, own_ref, dw_ref)
    center, inverse = normal_terms(s_ref, C, total_cells)
    gain, bias = gb_ref[0], gb_ref[1]

    def step(x, y, carry):
        normed = (h_ref[x, y] - center) * inverse
        slope = acc_ref[x, y + 2] * activate_slope(normed * gain + bias)
        o_ref[x, y] = slope
        return carry[0] + slope, carry[1] + slope * normed

    zero = jnp.zeros((C, Z), F32)
    t_ref[...] = pack_pair(*rows(X, Y, step, (zero, zero)))


def last_kernel(
    nx, ny, g_ref, v_ref, w_ref, d_ref, o_ref, both_ref, acc_ref, p_ref, send, recv, own_ref
):
    X, Y, C, Z = o_ref.shape
    fill_own(v_ref, own_ref)
    both_ref[9 * C :] = d_ref[...]
    dw_ref = both_ref.at[0 : 9 * C]
    conv_halo(nx, ny, True, g_ref, w_ref, acc_ref, p_ref, send, recv, own_ref, dw_ref)

    def step(x, y, carry):
        o_ref[x, y] = acc_ref[x, y + 2].astype(BF16)
        return carry

    rows(X, Y, step, 0)


def call(kernel, name, outs, *operands, scratch=(), collective=None):
    params = {}
    if collective is not None:
        params["compiler_params"] = pltpu.CompilerParams(
            collective_id=collective, has_side_effects=True
        )
    return pl.pallas_call(
        kernel,
        name=name,
        out_shape=[jax.ShapeDtypeStruct(s, d) for s, d in outs],
        in_specs=[VSPEC] * len(operands),
        out_specs=[VSPEC] * len(outs),
        scratch_shapes=list(scratch),
        **params,
    )(*operands)


def local(features, kernel_one, gain_one, bias_one, kernel_two, gain_two, bias_two, cotangent):
    C, X, Y, Z = features.shape
    nx, ny = lax.axis_size("gx"), lax.axis_size("gy")
    total_cells = float(X * Y * Z * nx * ny)
    full = (X, Y, C, Z)
    tall = (X, Y + 4, C, Z)
    stat = (8, 128)
    faces = [
        pltpu.VMEM(tall, F32),
        pltpu.VMEM((X + 2, Y + 2, C, Z), BF16),
        pltpu.SemaphoreType.DMA((6 + 2 * PIECES,)),
        pltpu.SemaphoreType.DMA((6 + 2 * PIECES,)),
    ]
    own = [pltpu.VMEM(tall, BF16)]
    forward = functools.partial(forward_kernel, nx, ny)

    def ahead(kernel):
        return jnp.transpose(kernel, (2, 3, 0, 4, 1)).reshape(9 * C, 3 * C)

    def behind(kernel):
        return jnp.transpose(kernel, (2, 3, 1, 4, 0)).reshape(9 * C, 3 * C)

    def rows_of(gain, bias):
        return jnp.broadcast_to(jnp.stack([gain, bias])[:, :, None], (2, C, Z))

    params_one, params_two = rows_of(gain_one, bias_one), rows_of(gain_two, bias_two)
    ft = jnp.transpose(features, (1, 2, 0, 3))
    ct = jnp.transpose(cotangent, (1, 2, 0, 3))

    h1, s1 = call(
        forward, "forward", [(full, F32), (stat, F32)], ft, ahead(kernel_one),
        scratch=faces, collective=0,
    )
    s1 = sum_stats(s1, nx, ny)
    (a,) = call(
        functools.partial(active_kernel, total_cells), "active", [(full, BF16)], h1, s1, params_one
    )
    h2, s2 = call(
        forward, "forward", [(full, F32), (stat, F32)], a, ahead(kernel_two),
        scratch=faces, collective=0,
    )
    s2 = sum_stats(s2, nx, ny)
    out, t2 = call(
        functools.partial(output_kernel, total_cells), "output", [(full, BF16), (stat, F32)],
        h2, s2, params_two, ct,
    )
    t2 = sum_stats(t2, nx, ny)
    (g2,) = call(
        functools.partial(gradient_kernel, total_cells, False), "grad_two", [(full, BF16)],
        h2, s2, params_two, ct, t2,
    )
    slope_one, t1, dw2 = call(
        functools.partial(back_kernel, total_cells, nx, ny), "back",
        [(full, F32), (stat, F32), ((9 * C, 128), F32)],
        g2, a, behind(kernel_two), h1, s1, params_one,
        scratch=faces + own, collective=3,
    )
    t1 = sum_stats(t1, nx, ny)
    (g1,) = call(
        functools.partial(gradient_kernel, total_cells, True), "grad_one", [(full, BF16)],
        h1, s1, params_one, slope_one, t1,
    )
    fg, dw = call(
        functools.partial(last_kernel, nx, ny), "last", [(full, BF16), ((18 * C, 128), F32)],
        g1, ft, behind(kernel_one), dw2, scratch=faces + own, collective=4,
    )
    summed = sum_weights(dw, nx, ny)
    scale = 1.0 / jnp.sqrt(jnp.float32(total_cells))

    def gradient_of(block):
        split = block[:, : 3 * C].reshape(3, 3, C, 3, C)
        return jnp.transpose(split, (4, 2, 0, 1, 3)) * scale

    norm_grads = jnp.stack([t1[1, :C], t1[0, :C], t2[1, :C], t2[0, :C]]) * scale
    return (
        jnp.transpose(out, (2, 0, 1, 3)),
        jnp.transpose(fg, (2, 0, 1, 3)),
        gradient_of(summed[: 9 * C]),
        gradient_of(summed[9 * C :]),
        norm_grads,
    )


def solution(mesh):
    in_specs = (P(None, "gx", "gy", None), P(), P(), P(), P(), P(), P(), P(None, "gx", "gy", None))
    out_specs = (P(None, "gx", "gy", None), P(None, "gx", "gy", None), P(), P(), P())
    return jax.shard_map(local, mesh=mesh, in_specs=in_specs, out_specs=out_specs, check_vma=False)
```
